32 devices in a mesh: shift: 4 (over y, core), band: 4 (over z), lane: 2 (over x).
Axes of the slice: x: 2, y: 2, z: 4, core: 2. Of those that a mesh axis runs over, the one named last changes fastest.
Arguments:
- source_terms: float32 [1024, 128, 128], P(('shift', 'band'), 'lane'), parts along dimension 0, may hold values from -6 to 6
- initial_values: float32 [1024, 128, 128], P(('shift', 'band'), 'lane'), parts along dimension 0, may hold values from -6 to 6
- absorption: float32 [1024, 128, 128], P(('shift', 'band'), 'lane'), parts along dimension 0, may hold values from 0.1 to 0.9
Outputs:
- corrected: float32 [1024, 128, 128], P(('shift', 'band'), 'lane'), parts along dimension 0
The draws below stay inside these ranges and needn't reach their ends.
There are 4 independent parts, one for each index of `shift`. The reference program is written for one: setup_inputs(seed, part) draws one part's arguments, and reference() takes and returns one part's arrays. A program takes and returns all parts, laid end to end along the dimension named above; each array names one. Nothing has to cross between parts.
All inputs are finite; a program needn't handle non-finite values.
Results may differ from the reference program's by a relative error of at most 0.0003.
Values sent between devices are 32-bit elements.
A program may use at most 64 MiB of HBM per device.

```python
import jax
import jax.numpy as jnp
from jax import lax

CASES = 128
RATIO = 2
BEFORE = 3
AFTER = 3
INNER = 13
GRID_Y = 256
GRID_X = 128


def level_of(key, extent, pieces, low, largest):
    loudness, own = 1.0, jax.random.fold_in(key, 6)
    for axis_at, shards_of in pieces:
        heights = jnp.exp(jax.random.uniform(jax.random.fold_in(own, axis_at), (shards_of,), jnp.float32, low / len(pieces), largest / len(pieces)))
        loudness = loudness * jnp.repeat(heights, extent[axis_at] // shards_of).reshape([-1 if axis == axis_at else 1 for axis in range(len(extent))])
    return loudness


def noise(stream_key, extent, spread, bound, split=(), held_as=jnp.bfloat16):
    drawn = spread * jax.random.normal(stream_key, extent, jnp.float32)
    if split:
        drawn = drawn * level_of(stream_key, extent, split, -0.22, 0.18)
    return jnp.clip(drawn, -bound, bound).astype(held_as)


def setup_inputs(seed: int = 0, part: int = 0) -> dict:
    arg_keys = jax.random.split(jax.random.key(seed), 4)
    part_keys = jax.random.split(jax.random.fold_in(arg_keys[3], part), 4)
    source_terms = noise(part_keys[0], (GRID_Y, GRID_X, CASES), 1.0, 6.0, ((0, 4), (1, 2)), jnp.float32)
    initial_values = noise(part_keys[1], (GRID_Y, GRID_X, CASES), 1.0, 6.0, ((0, 4), (1, 2)), jnp.float32)
    absorption = jnp.clip(0.1 + 0.79999997 * jax.random.uniform(part_keys[2], (GRID_Y, GRID_X, CASES), jnp.float32) ** level_of(part_keys[2], (GRID_Y, GRID_X, CASES), ((0, 4), (1, 2)), -0.2, 0.2), 0.1, 0.9)
    return {"source_terms": source_terms, "initial_values": initial_values, "absorption": absorption}


def neighbour_sum(padded):
    inner_y, inner_x = padded.shape[0] - 2, padded.shape[1] - 2
    middle_rows = lax.slice_in_dim(padded, 1, 1 + inner_y, axis=0)
    middle_columns = lax.slice_in_dim(padded, 1, 1 + inner_x, axis=1)
    return (lax.slice_in_dim(middle_columns, 0, inner_y, axis=0) + lax.slice_in_dim(middle_columns, 2, 2 + inner_y, axis=0)
            + lax.slice_in_dim(middle_rows, 0, inner_x, axis=1) + lax.slice_in_dim(middle_rows, 2, 2 + inner_x, axis=1))


def sweep_once(padded, values, load, mass_here):
    return values + 0.8 * (load + neighbour_sum(padded) - (4.0 + mass_here) * values) / (4.0 + mass_here)


def block_means(values):
    cut = values.reshape(values.shape[0] // RATIO, RATIO, values.shape[1] // RATIO, RATIO, values.shape[2])
    return jnp.mean(cut, axis=(1, 3))


def spread_blocks(values):
    return jnp.repeat(jnp.repeat(values, RATIO, axis=0), RATIO, axis=1)


def reference(source_terms, initial_values, absorption):
    values = initial_values
    for sweep in range(BEFORE):
        values = sweep_once(jnp.pad(values, ((1, 1), (1, 1), (0, 0)), mode="constant"), values, source_terms, absorption)
    defect = source_terms + neighbour_sum(jnp.pad(values, ((1, 1), (1, 1), (0, 0)), mode="constant")) - (4.0 + absorption) * values
    coarse_load, coarse_mass = block_means(defect) * RATIO, block_means(absorption) * RATIO
    coarse_values = jnp.zeros_like(coarse_load)
    for sweep in range(INNER):
        coarse_values = sweep_once(jnp.pad(coarse_values, ((1, 1), (1, 1), (0, 0)), mode="constant"), coarse_values, coarse_load, coarse_mass)
    values = values + spread_blocks(coarse_values)
    for sweep in range(AFTER):
        values = sweep_once(jnp.pad(values, ((1, 1), (1, 1), (0, 0)), mode="constant"), values, source_terms, absorption)
    corrected = values
    return corrected
```

```python
import functools

import jax
import jax.numpy as jnp
from jax import lax
from jax.experimental import pallas as pl
from jax.experimental.pallas import tpu as pltpu
from jax.sharding import PartitionSpec as P

RATIO = 2
BEFORE = 3
AFTER = 3
INNER = 13
HALO = 8
ROWS = 2
SUB = 8
MESH = pl.DeviceIdType.MESH
DIRS = [(-1, 0), (1, 0), (0, -1), (0, 1), (-1, -1), (-1, 1), (1, -1), (1, 1)]

TRADES = [
    ("u_first", "fine", 2),
    ("w", "fine", 1),
    ("f", "fine", 1),
    ("cw", "coarse", 7),
    ("u_second", "fine", 2),
    ("cf", "coarse", 7),
    ("cu", "coarse", 6),
    ("u_third", "fine", 2),
]


class Grid:
    def __init__(self, rows, columns, row_halo, column_halo):
        self.rows, self.columns = rows, columns
        self.row_halo, self.column_halo = row_halo, column_halo
        self.pieces = (columns + 2 * column_halo) // SUB
        self.width = self.pieces * SUB
        self.stored = (rows + 2 * row_halo) * self.width

    def at(self, column):
        return (column % self.pieces) * SUB + column // self.pieces


def kernel(grids, src_hbm, init_hbm, abs_hbm, out_hbm, *scratch):
    fine, coarse = grids["fine"], grids["coarse"]
    raw = scratch[:3]
    u, v, w, f, iw, out, cw, cf, ca, cb, in_sem, out_sem, send_sem, recv_sem = scratch[3:17]
    lands = scratch[17:]
    band, lane = lax.axis_index("band"), lax.axis_index("lane")
    bands, lanes = lax.axis_size("band"), lax.axis_size("lane")

    def exists(q):
        dy, dx = q
        there = jnp.bool_(True)
        if dy:
            there = (band > 0) if dy < 0 else (band < bands - 1)
        if dx:
            beside = (lane > 0) if dx < 0 else (lane < lanes - 1)
            there = beside if not dy else there & beside
        return there

    def name_of(q):
        return {"band": band + q[0], "lane": lane + q[1]}

    loads = [
        pltpu.make_async_copy(
            ref, raw[i].at[:, pl.ds(fine.column_halo, fine.columns), :], in_sem.at[i]
        )
        for i, ref in enumerate((abs_hbm, src_hbm, init_hbm))
    ]
    for copy in loads:
        copy.start()

    trades = {}
    for t, (name, which, depth) in enumerate(TRADES):
        trades[name] = (t, grids[which], depth) + tuple(lands[4 * t : 4 * t + 4])

    barrier = pltpu.get_barrier_semaphore()
    for q in DIRS:
        @pl.when(exists(q))
        def _():
            pl.semaphore_signal(barrier, inc=1, device_id=name_of(q), device_id_type=MESH)

    def landing(trade, q):
        t, g, depth, strips, rows, columns, corners = trade
        dy, dx = q
        if not dx:
            return rows.at[(dy + 1) // 2]
        if not dy:
            return columns.at[(dx + 1) // 2]
        return corners.at[(dy + 1) // 2 * 2 + (dx + 1) // 2]

    def source(trade, arr, q):
        t, g, depth, strips, rows, columns, corners = trade
        dy, dx = q
        if not dx:
            first = g.row_halo if dy < 0 else g.row_halo + g.rows - depth
            return arr.at[pl.ds(first * g.width, depth * g.width), :]
        strip = strips.at[(dx + 1) // 2]
        if not dy:
            return strip
        return strip.at[:, pl.ds(0 if dy < 0 else g.rows - SUB, SUB), :]

    for trade in trades.values():
        for q in DIRS:
            @pl.when(jnp.logical_not(exists(q)))
            def _():
                ref = landing(trade, q)
                ref[...] = jnp.zeros(ref.shape, jnp.float32)

    on_band = (band > 0).astype(jnp.int32) + (band < bands - 1).astype(jnp.int32)
    on_lane = (lane > 0).astype(jnp.int32) + (lane < lanes - 1).astype(jnp.int32)
    pl.semaphore_wait(barrier, (on_band + 1) * (on_lane + 1) - 1)

    def copy_of(trade, arr, q, arriving):
        t = trade[0]
        back = (-q[0], -q[1])
        i, j = DIRS.index(q), DIRS.index(back)
        return pltpu.make_async_remote_copy(
            src_ref=source(trade, arr, q if not arriving else back),
            dst_ref=landing(trade, back if not arriving else q),
            send_sem=send_sem.at[t * 8 + i],
            recv_sem=recv_sem.at[t * 8 + (i if arriving else j)],
            device_id=name_of(q),
            device_id_type=MESH,
        )

    def send(name, arr):
        trade = trades[name]
        t, g, depth, strips, rows, columns, corners = trade
        for q in DIRS[:2]:
            @pl.when(exists(q))
            def _():
                copy_of(trade, arr, q, False).start()
        for side in range(2):
            first = g.column_halo if side == 0 else g.column_halo + g.columns - depth
            for j in range(depth):
                for i in range(g.rows // SUB):
                    at = (g.row_halo + SUB * i) * g.width + g.at(first + j)
                    strips[side, j, pl.ds(SUB * i, SUB), :] = arr[
                        pl.ds(at, SUB, stride=g.width), :
                    ]
        for q in DIRS[2:]:
            @pl.when(exists(q))
            def _():
                copy_of(trade, arr, q, False).start()

    def receive(name, arr):
        trade = trades[name]
        t, g, depth, strips, rows, columns, corners = trade
        for q in DIRS:
            @pl.when(exists(q))
            def _():
                copy_of(trade, arr, q, False).wait_send()
                copy_of(trade, arr, q, True).wait_recv()
        for side in range(2):
            first = g.row_halo - depth if side == 0 else g.row_halo + g.rows
            arr[pl.ds(first * g.width, depth * g.width), :] = rows[side]
        for side in range(2):
            first = g.column_halo - depth if side == 0 else g.column_halo + g.columns
            for j in range(depth):
                place = g.at(first + j)
                for i in range(g.rows // SUB):
                    at = (g.row_halo + SUB * i) * g.width + place
                    arr[pl.ds(at, SUB, stride=g.width), :] = columns[
                        side, j, pl.ds(SUB * i, SUB), :
                    ]
                for end in range(2):
                    row = g.row_halo - depth if end == 0 else g.row_halo + g.rows
                    skip = SUB - depth if end == 0 else 0
                    arr[pl.ds(row * g.width + place, depth, stride=g.width), :] = corners[
                        end * 2 + side, j, pl.ds(skip, depth), :
                    ]

    def piece(ref, g, row, k):
        return ref[pl.ds(pl.multiple_of(row * g.width + k * SUB, SUB), SUB), :]

    def put(ref, g, row, k, value):
        ref[pl.ds(pl.multiple_of(row * g.width + k * SUB, SUB), SUB), :] = value

    def around(ref, g, row):
        here = [piece(ref, g, row, k) for k in range(g.pieces)]
        before = [pltpu.roll(here[-1], 1, 0)] + here[:-1]
        after = here[1:] + [pltpu.roll(here[0], SUB - 1, 0)]
        sums = [
            (piece(ref, g, row - 1, k) + piece(ref, g, row + 1, k)) + (before[k] + after[k])
            for k in range(g.pieces)
        ]
        return here, sums

    def sweep(g, old, new, weight, load, wider):
        @pl.loop(g.row_halo - wider, g.row_halo + g.rows + wider, unroll=2)
        def _(row):
            here, sums = around(old, g, row)
            for k in range(g.pieces):
                value = (
                    0.2 * here[k] + piece(load, g, row, k) + piece(weight, g, row, k) * sums[k]
                )
                if new is out:
                    new[pl.ds((row - g.row_halo) * g.width + k, SUB, stride=g.pieces), :] = value
                else:
                    put(new, g, row, k, value)

    loads[0].wait()

    @pl.loop(0, coarse.rows)
    def _(row):
        total = [0.0] * coarse.pieces
        for half in range(RATIO):
            at = RATIO * row + half
            for k in range(fine.pieces):
                g4 = 4.0 + raw[0][at, pl.ds(k, SUB, stride=fine.pieces), :]
                put(w, fine, at + fine.row_halo, k, 0.8 / g4)
                put(iw, fine, at, k, 1.25 * g4)
                total[k // RATIO] = total[k // RATIO] + g4
        for k in range(coarse.pieces):
            mean = total[k] * (1.0 / RATIO) - (4.0 * RATIO - 4.0)
            put(cw, coarse, row + coarse.row_halo, k, 0.8 / mean)

    send("w", w)
    loads[2].wait()

    @pl.loop(0, fine.rows, unroll=2)
    def _(row):
        for k in range(fine.pieces):
            put(u, fine, row + fine.row_halo, k, raw[2][row, pl.ds(k, SUB, stride=fine.pieces), :])

    send("u_first", u)
    loads[1].wait()

    @pl.loop(0, fine.rows, unroll=2)
    def _(row):
        for k in range(fine.pieces):
            at = row + fine.row_halo
            put(f, fine, at, k, piece(w, fine, at, k) * raw[1][row, pl.ds(k, SUB, stride=fine.pieces), :])

    send("f", f)
    send("cw", cw)
    receive("w", w)
    receive("u_first", u)
    receive("f", f)
    sweep(fine, u, v, w, f, 1)
    sweep(fine, v, u, w, f, 0)
    send("u_second", u)
    receive("u_second", u)
    sweep(fine, u, v, w, f, 1)

    @pl.loop(0, coarse.rows)
    def _(row):
        total = [0.0] * coarse.pieces
        for half in range(RATIO):
            at = RATIO * row + half + fine.row_halo
            here, sums = around(v, fine, at)
            for k in range(fine.pieces):
                change = piece(f, fine, at, k) + piece(w, fine, at, k) * sums[k] - 0.8 * here[k]
                total[k // RATIO] = total[k // RATIO] + change * piece(
                    iw, fine, at - fine.row_halo, k
                )
        for k in range(coarse.pieces):
            at = row + coarse.row_halo
            put(cf, coarse, at, k, total[k] * (1.0 / RATIO) * piece(cw, coarse, at, k))

    send("cf", cf)
    receive("cw", cw)
    receive("cf", cf)
    old, new, spare = cf, ca, cb
    left = INNER - 1
    wider = 7
    while wider > 0:
        wider -= 1
        sweep(coarse, old, new, cw, cf, wider)
        old, new, spare = new, spare, new
        left -= 1
    send("cu", old)
    receive("cu", old)
    new = ca if old is cb else cb
    wider = 6
    while left > 0:
        wider -= 1
        sweep(coarse, old, new, cw, cf, wider)
        old, new = new, old
        left -= 1

    @pl.loop(-1, coarse.rows + 1)
    def _(row):
        for k in range(coarse.pieces):
            more = piece(old, coarse, row + coarse.row_halo, k)
            for half in range(RATIO):
                at = RATIO * row + half + fine.row_halo
                for part in range(RATIO):
                    put(v, fine, at, RATIO * k + part, piece(v, fine, at, RATIO * k + part) + more)

    sweep(fine, v, u, w, f, 0)
    send("u_third", u)
    receive("u_third", u)
    sweep(fine, u, v, w, f, 1)
    sweep(fine, v, out, w, f, 0)
    store = pltpu.make_async_copy(
        out.reshape(fine.rows, fine.width, 128).at[:, pl.ds(fine.column_halo, fine.columns), :],
        out_hbm,
        out_sem,
    )
    store.start()
    store.wait()


def per_device(source_terms, initial_values, absorption):
    rows, columns, cases = source_terms.shape
    fine = Grid(rows, columns, ROWS, RATIO * HALO)
    coarse = Grid(rows // RATIO, columns // RATIO, HALO, HALO)
    grids = {"fine": fine, "coarse": coarse}

    def held(*shape):
        return pltpu.VMEM(shape + (cases,), jnp.float32)

    shapes = [held(rows, fine.width) for _ in range(3)]
    shapes += [held(fine.stored) for _ in range(4)]
    shapes += [held(rows * fine.width), held(rows * fine.width)]
    shapes += [held(coarse.stored) for _ in range(4)]
    count = len(TRADES) * len(DIRS)
    shapes += [
        pltpu.SemaphoreType.DMA((3,)),
        pltpu.SemaphoreType.DMA,
        pltpu.SemaphoreType.DMA((count,)),
        pltpu.SemaphoreType.DMA((count,)),
    ]
    for name, which, depth in TRADES:
        g = grids[which]
        shapes += [
            held(2, depth, g.rows),
            held(2, depth * g.width),
            held(2, depth, g.rows),
            held(4, depth, SUB),
        ]
    return pl.pallas_call(
        functools.partial(kernel, grids),
        out_shape=jax.ShapeDtypeStruct(source_terms.shape, jnp.float32),
        in_specs=[pl.BlockSpec(memory_space=pl.ANY)] * 3,
        out_specs=pl.BlockSpec(memory_space=pl.ANY),
        scratch_shapes=shapes,
        compiler_params=pltpu.CompilerParams(
            collective_id=0, has_side_effects=True, vmem_limit_bytes=60 * 1024 * 1024
        ),
    )(source_terms, initial_values, absorption)


def solution(mesh):
    placed = P(("shift", "band"), "lane", None)
    return jax.shard_map(
        per_device,
        mesh=mesh,
        in_specs=(placed, placed, placed),
        out_specs=placed,
        check_vma=False,
    )
```

```python
import functools

import jax
import jax.numpy as jnp
from jax import lax
from jax.experimental import pallas as pl
from jax.experimental.pallas import tpu as pltpu
from jax.sharding import PartitionSpec as P

RATIO = 2
BEFORE = 3
AFTER = 3
INNER = 13
HALO = 8
ROWS = 2
SUB = 8
MESH = pl.DeviceIdType.MESH
DIRS = [(-1, 0), (1, 0), (0, -1), (0, 1), (-1, -1), (-1, 1), (1, -1), (1, 1)]

TRADES = [
    ("u_first", "fine", 2),
    ("w", "fine", 1),
    ("f", "fine", 1),
    ("cw", "coarse", 7),
    ("u_second", "fine", 2),
    ("cf", "coarse", 7),
    ("cu", "coarse", 6),
    ("u_third", "fine", 2),
]


class Grid:
    def __init__(self, rows, columns, row_halo, column_halo):
        self.rows, self.columns = rows, columns
        self.row_halo, self.column_halo = row_halo, column_halo
        self.pieces = (columns + 2 * column_halo) // SUB
        self.width = self.pieces * SUB
        self.stored = (rows + 2 * row_halo) * self.width

    def at(self, column):
        return (column % self.pieces) * SUB + column // self.pieces


def kernel(grids, src_hbm, init_hbm, abs_hbm, out_hbm, *scratch):
    fine, coarse = grids["fine"], grids["coarse"]
    raw = scratch[:3]
    u, v, w, f, iw, out, cw, cf, ca, cb, in_sem, out_sem, send_sem, recv_sem = scratch[3:17]
    lands = scratch[17:]
    band, lane = lax.axis_index("band"), lax.axis_index("lane")
    bands, lanes = lax.axis_size("band"), lax.axis_size("lane")

    def exists(q):
        dy, dx = q
        there = jnp.bool_(True)
        if dy:
            there = (band > 0) if dy < 0 else (band < bands - 1)
        if dx:
            beside = (lane > 0) if dx < 0 else (lane < lanes - 1)
            there = beside if not dy else there & beside
        return there

    def name_of(q):
        return {"band": band + q[0], "lane": lane + q[1]}

    loads = [
        pltpu.make_async_copy(
            ref,
            raw[i].reshape(fine.rows, fine.width, 128).at[:, pl.ds(fine.column_halo, fine.columns), :],
            in_sem.at[i],
        )
        for i, ref in enumerate((abs_hbm, src_hbm, init_hbm))
    ]
    for i in (2, 0, 1):
        loads[i].start()

    trades = {}
    for t, (name, which, depth) in enumerate(TRADES):
        trades[name] = (t, grids[which], depth) + tuple(lands[5 * t : 5 * t + 5])

    barrier = pltpu.get_barrier_semaphore()
    for q in DIRS:
        @pl.when(exists(q))
        def _():
            pl.semaphore_signal(barrier, inc=1, device_id=name_of(q), device_id_type=MESH)

    def landing(trade, q):
        t, g, depth, sides, strips, rows, columns, corners = trade
        dy, dx = q
        if not dx:
            return rows.at[(dy + 1) // 2, :, pl.ds(g.column_halo, g.columns), :]
        if not dy:
            return columns.at[(dx + 1) // 2]
        return corners.at[(dy + 1) // 2 * 2 + (dx + 1) // 2]

    def source(trade, q):
        t, g, depth, sides, strips, rows, columns, corners = trade
        dy, dx = q
        if not dx:
            return sides.at[(dy + 1) // 2, :, pl.ds(g.column_halo, g.columns), :]
        strip = strips.at[(dx + 1) // 2]
        if not dy:
            return strip
        return strip.at[:, pl.ds(0 if dy < 0 else g.rows - SUB, SUB), :]

    for trade in trades.values():
        for q in DIRS:
            @pl.when(jnp.logical_not(exists(q)))
            def _():
                ref = landing(trade, q)
                ref[...] = jnp.zeros(ref.shape, jnp.float32)

    on_band = (band > 0).astype(jnp.int32) + (band < bands - 1).astype(jnp.int32)
    on_lane = (lane > 0).astype(jnp.int32) + (lane < lanes - 1).astype(jnp.int32)
    pl.semaphore_wait(barrier, (on_band + 1) * (on_lane + 1) - 1)

    def copy_of(trade, q, arriving):
        t = trade[0]
        back = (-q[0], -q[1])
        i, j = DIRS.index(q), DIRS.index(back)
        return pltpu.make_async_remote_copy(
            src_ref=source(trade, q if not arriving else back),
            dst_ref=landing(trade, back if not arriving else q),
            send_sem=send_sem.at[t * 8 + i],
            recv_sem=recv_sem.at[t * 8 + (i if arriving else j)],
            device_id=name_of(q),
            device_id_type=MESH,
        )

    def start(trade, directions):
        for q in directions:
            @pl.when(exists(q))
            def _():
                copy_of(trade, q, False).start()

    def send(name, arr):
        trade = trades[name]
        t, g, depth, sides, strips, rows, columns, corners = trade
        for side in range(2):
            first = g.row_halo if side == 0 else g.row_halo + g.rows - depth
            for i in range(depth):
                for k in range(g.pieces):
                    sides[side, i, pl.ds(k, SUB, stride=g.pieces), :] = piece(arr, g, first + i, k)
        start(trade, DIRS[:2])
        for side in range(2):
            first = g.column_halo if side == 0 else g.column_halo + g.columns - depth
            for j in range(depth):
                for i in range(g.rows // SUB):
                    at = (g.row_halo + SUB * i) * g.width + g.at(first + j)
                    strips[side, j, pl.ds(SUB * i, SUB), :] = arr[
                        pl.ds(at, SUB, stride=g.width), :
                    ]
        start(trade, DIRS[2:])

    def send_raw(name, value):
        trade = trades[name]
        t, g, depth, sides, strips, rows, columns, corners = trade
        for side in range(2):
            first = 0 if side == 0 else g.rows - depth
            for i in range(depth):
                for c in range(g.columns // SUB):
                    at = g.column_halo + SUB * c
                    sides[side, i, pl.ds(at, SUB), :] = value(
                        lambda ref: ref[pl.ds((first + i) * g.width + at, SUB), :]
                    )
        start(trade, DIRS[:2])
        for side in range(2):
            first = g.column_halo if side == 0 else g.column_halo + g.columns - depth
            for j in range(depth):
                for i in range(g.rows // SUB):
                    strips[side, j, pl.ds(SUB * i, SUB), :] = value(
                        lambda ref: ref[pl.ds(SUB * i * g.width + first + j, SUB, stride=g.width), :]
                    )
        start(trade, DIRS[2:])

    def receive(name, arr):
        trade = trades[name]
        t, g, depth, sides, strips, rows, columns, corners = trade
        for q in DIRS:
            @pl.when(exists(q))
            def _():
                copy_of(trade, q, False).wait_send()
                copy_of(trade, q, True).wait_recv()
        for side in range(2):
            first = g.row_halo - depth if side == 0 else g.row_halo + g.rows
            for i in range(depth):
                for k in range(g.pieces):
                    put(arr, g, first + i, k, rows[side, i, pl.ds(k, SUB, stride=g.pieces), :])
        for side in range(2):
            first = g.column_halo - depth if side == 0 else g.column_halo + g.columns
            for j in range(depth):
                place = g.at(first + j)
                for i in range(g.rows // SUB):
                    at = (g.row_halo + SUB * i) * g.width + place
                    arr[pl.ds(at, SUB, stride=g.width), :] = columns[
                        side, j, pl.ds(SUB * i, SUB), :
                    ]
                for end in range(2):
                    row = g.row_halo - depth if end == 0 else g.row_halo + g.rows
                    skip = SUB - depth if end == 0 else 0
                    arr[pl.ds(row * g.width + place, depth, stride=g.width), :] = corners[
                        end * 2 + side, j, pl.ds(skip, depth), :
                    ]

    def piece(ref, g, row, k):
        return ref[pl.ds(pl.multiple_of(row * g.width + k * SUB, SUB), SUB), :]

    def put(ref, g, row, k, value):
        ref[pl.ds(pl.multiple_of(row * g.width + k * SUB, SUB), SUB), :] = value

    def around(ref, g, row):
        here = [piece(ref, g, row, k) for k in range(g.pieces)]
        before = [pltpu.roll(here[-1], 1, 0)] + here[:-1]
        after = here[1:] + [pltpu.roll(here[0], SUB - 1, 0)]
        sums = [
            (piece(ref, g, row - 1, k) + piece(ref, g, row + 1, k)) + (before[k] + after[k])
            for k in range(g.pieces)
        ]
        return here, sums

    def sweep(g, old, new, weight, load, wider):
        @pl.loop(g.row_halo - wider, g.row_halo + g.rows + wider, unroll=2)
        def _(row):
            here, sums = around(old, g, row)
            for k in range(g.pieces):
                value = (
                    0.2 * here[k] + piece(load, g, row, k) + piece(weight, g, row, k) * sums[k]
                )
                if new is out:
                    new[pl.ds((row - g.row_halo) * g.width + k, SUB, stride=g.pieces), :] = value
                else:
                    put(new, g, row, k, value)

    loads[2].wait()
    send_raw("u_first", lambda read: read(raw[2]))
    loads[0].wait()
    send_raw("w", lambda read: 0.8 / (4.0 + read(raw[0])))
    loads[1].wait()
    send_raw("f", lambda read: 0.8 / (4.0 + read(raw[0])) * read(raw[1]))

    @pl.loop(0, coarse.rows)
    def _(row):
        total = [0.0] * coarse.pieces
        for half in range(RATIO):
            at = RATIO * row + half
            for k in range(fine.pieces):
                g4 = 4.0 + raw[0][pl.ds(at * fine.width + k, SUB, stride=fine.pieces), :]
                put(w, fine, at + fine.row_halo, k, 0.8 / g4)
                put(iw, fine, at, k, 1.25 * g4)
                total[k // RATIO] = total[k // RATIO] + g4
        for k in range(coarse.pieces):
            mean = total[k] * (1.0 / RATIO) - (4.0 * RATIO - 4.0)
            put(cw, coarse, row + coarse.row_halo, k, 0.8 / mean)

    send("cw", cw)

    @pl.loop(0, fine.rows, unroll=2)
    def _(row):
        for k in range(fine.pieces):
            put(u, fine, row + fine.row_halo, k, raw[2][pl.ds(row * fine.width + k, SUB, stride=fine.pieces), :])


    @pl.loop(0, fine.rows, unroll=2)
    def _(row):
        for k in range(fine.pieces):
            at = row + fine.row_halo
            put(f, fine, at, k, piece(w, fine, at, k) * raw[1][pl.ds(row * fine.width + k, SUB, stride=fine.pieces), :])

    receive("w", w)
    receive("u_first", u)
    receive("f", f)
    sweep(fine, u, v, w, f, 1)
    sweep(fine, v, u, w, f, 0)
    send("u_second", u)
    receive("u_second", u)
    sweep(fine, u, v, w, f, 1)

    @pl.loop(0, coarse.rows)
    def _(row):
        total = [0.0] * coarse.pieces
        for half in range(RATIO):
            at = RATIO * row + half + fine.row_halo
            here, sums = around(v, fine, at)
            for k in range(fine.pieces):
                change = piece(f, fine, at, k) + piece(w, fine, at, k) * sums[k] - 0.8 * here[k]
                total[k // RATIO] = total[k // RATIO] + change * piece(
                    iw, fine, at - fine.row_halo, k
                )
        for k in range(coarse.pieces):
            at = row + coarse.row_halo
            put(cf, coarse, at, k, total[k] * (1.0 / RATIO) * piece(cw, coarse, at, k))

    send("cf", cf)
    receive("cw", cw)
    receive("cf", cf)
    old, new, spare = cf, ca, cb
    left = INNER - 1
    wider = 7
    while wider > 0:
        wider -= 1
        sweep(coarse, old, new, cw, cf, wider)
        old, new, spare = new, spare, new
        left -= 1
    send("cu", old)
    receive("cu", old)
    new = ca if old is cb else cb
    wider = 6
    while left > 0:
        wider -= 1
        sweep(coarse, old, new, cw, cf, wider)
        old, new = new, old
        left -= 1

    @pl.loop(-1, coarse.rows + 1)
    def _(row):
        for k in range(coarse.pieces):
            more = piece(old, coarse, row + coarse.row_halo, k)
            for half in range(RATIO):
                at = RATIO * row + half + fine.row_halo
                for part in range(RATIO):
                    put(v, fine, at, RATIO * k + part, piece(v, fine, at, RATIO * k + part) + more)

    sweep(fine, v, u, w, f, 0)
    send("u_third", u)
    receive("u_third", u)
    sweep(fine, u, v, w, f, 1)
    sweep(fine, v, out, w, f, 0)
    store = pltpu.make_async_copy(
        out.reshape(fine.rows, fine.width, 128).at[:, pl.ds(fine.column_halo, fine.columns), :],
        out_hbm,
        out_sem,
    )
    store.start()
    store.wait()


def per_device(source_terms, initial_values, absorption):
    rows, columns, cases = source_terms.shape
    fine = Grid(rows, columns, ROWS, RATIO * HALO)
    coarse = Grid(rows // RATIO, columns // RATIO, HALO, HALO)
    grids = {"fine": fine, "coarse": coarse}

    def held(*shape):
        return pltpu.VMEM(shape + (cases,), jnp.float32)

    shapes = [held(rows * fine.width) for _ in range(3)]
    shapes += [held(fine.stored) for _ in range(4)]
    shapes += [held(rows * fine.width), held(rows * fine.width)]
    shapes += [held(coarse.stored) for _ in range(4)]
    count = len(TRADES) * len(DIRS)
    shapes += [
        pltpu.SemaphoreType.DMA((3,)),
        pltpu.SemaphoreType.DMA,
        pltpu.SemaphoreType.DMA((count,)),
        pltpu.SemaphoreType.DMA((count,)),
    ]
    for name, which, depth in TRADES:
        g = grids[which]
        shapes += [
            held(2, depth, g.width),
            held(2, depth, g.rows),
            held(2, depth, g.width),
            held(2, depth, g.rows),
            held(4, depth, SUB),
        ]
    return pl.pallas_call(
        functools.partial(kernel, grids),
        out_shape=jax.ShapeDtypeStruct(source_terms.shape, jnp.float32),
        in_specs=[pl.BlockSpec(memory_space=pl.ANY)] * 3,
        out_specs=pl.BlockSpec(memory_space=pl.ANY),
        scratch_shapes=shapes,
        compiler_params=pltpu.CompilerParams(
            collective_id=0, has_side_effects=True, vmem_limit_bytes=60 * 1024 * 1024
        ),
    )(source_terms, initial_values, absorption)


def solution(mesh):
    placed = P(("shift", "band"), "lane", None)
    return jax.shard_map(
        per_device,
        mesh=mesh,
        in_specs=(placed, placed, placed),
        out_specs=placed,
        check_vma=False,
    )
```

```python
import functools

import jax
import jax.numpy as jnp
from jax import lax
from jax.experimental import pallas as pl
from jax.experimental.pallas import tpu as pltpu
from jax.sharding import PartitionSpec as P

RATIO = 2
BEFORE = 3
AFTER = 3
INNER = 13
HALO = 8
ROWS = 2
SUB = 8
MESH = pl.DeviceIdType.MESH
CHUNKS = 4
BLOCK = 4
DIRS = [(-1, 0), (1, 0), (0, -1), (0, 1), (-1, -1), (-1, 1), (1, -1), (1, 1)]

TRADES = [
    ("u_first", "fine", 2),
    ("w", "fine", 1),
    ("f", "fine", 1),
    ("cw", "coarse", 7),
    ("u_second", "fine", 2),
    ("cf", "coarse", 7),
    ("cu", "coarse", 6),
    ("u_third", "fine", 2),
]


class Grid:
    def __init__(self, rows, columns, row_halo, column_halo):
        self.rows, self.columns = rows, columns
        self.row_halo, self.column_halo = row_halo, column_halo
        self.pieces = (columns + 2 * column_halo) // SUB
        self.width = self.pieces * SUB
        self.stored = (rows + 2 * row_halo) * self.width

    def at(self, column):
        return (column % self.pieces) * SUB + column // self.pieces


def kernel(grids, src_hbm, init_hbm, abs_hbm, out_hbm, *scratch):
    fine, coarse = grids["fine"], grids["coarse"]
    raw = scratch[:3]
    u, v, w, f, iw, out, cw, cf, ca, cb, in_sem, out_sem, send_sem, recv_sem = scratch[3:17]
    lands = scratch[17:]
    band, lane = lax.axis_index("band"), lax.axis_index("lane")
    bands, lanes = lax.axis_size("band"), lax.axis_size("lane")

    def exists(q):
        dy, dx = q
        there = jnp.bool_(True)
        if dy:
            there = (band > 0) if dy < 0 else (band < bands - 1)
        if dx:
            beside = (lane > 0) if dx < 0 else (lane < lanes - 1)
            there = beside if not dy else there & beside
        return there

    def name_of(q):
        return {"band": band + q[0], "lane": lane + q[1]}

    loads = [
        pltpu.make_async_copy(
            ref,
            raw[i].reshape(fine.rows, fine.width, 128).at[:, pl.ds(fine.column_halo, fine.columns), :],
            in_sem.at[i],
        )
        for i, ref in enumerate((abs_hbm, src_hbm, init_hbm))
    ]
    for i in (2, 0, 1):
        loads[i].start()

    trades = {}
    for t, (name, which, depth) in enumerate(TRADES):
        trades[name] = (t, grids[which], depth) + tuple(lands[5 * t : 5 * t + 5])

    barrier = pltpu.get_barrier_semaphore()
    for q in DIRS:
        @pl.when(exists(q))
        def _():
            pl.semaphore_signal(barrier, inc=1, device_id=name_of(q), device_id_type=MESH)

    def landing(trade, q):
        t, g, depth, sides, strips, rows, columns, corners = trade
        dy, dx = q
        if not dx:
            return rows.at[(dy + 1) // 2, :, pl.ds(g.column_halo, g.columns), :]
        if not dy:
            return columns.at[(dx + 1) // 2]
        return corners.at[(dy + 1) // 2 * 2 + (dx + 1) // 2]

    def source(trade, q):
        t, g, depth, sides, strips, rows, columns, corners = trade
        dy, dx = q
        if not dx:
            return sides.at[(dy + 1) // 2, :, pl.ds(g.column_halo, g.columns), :]
        strip = strips.at[(dx + 1) // 2]
        if not dy:
            return strip
        return strip.at[:, pl.ds(0 if dy < 0 else g.rows - SUB, SUB), :]

    for trade in trades.values():
        for q in DIRS:
            @pl.when(jnp.logical_not(exists(q)))
            def _():
                ref = landing(trade, q)
                ref[...] = jnp.zeros(ref.shape, jnp.float32)

    on_band = (band > 0).astype(jnp.int32) + (band < bands - 1).astype(jnp.int32)
    on_lane = (lane > 0).astype(jnp.int32) + (lane < lanes - 1).astype(jnp.int32)
    pl.semaphore_wait(barrier, (on_band + 1) * (on_lane + 1) - 1)

    def copy_of(trade, q, arriving):
        t = trade[0]
        back = (-q[0], -q[1])
        i, j = DIRS.index(q), DIRS.index(back)
        return pltpu.make_async_remote_copy(
            src_ref=source(trade, q if not arriving else back),
            dst_ref=landing(trade, back if not arriving else q),
            send_sem=send_sem.at[t * 8 + i],
            recv_sem=recv_sem.at[t * 8 + (i if arriving else j)],
            device_id=name_of(q),
            device_id_type=MESH,
        )

    def start(trade, directions):
        for q in directions:
            @pl.when(exists(q))
            def _():
                copy_of(trade, q, False).start()

    def send(name, arr):
        trade = trades[name]
        t, g, depth, sides, strips, rows, columns, corners = trade
        for side in range(2):
            first = g.column_halo if side == 0 else g.column_halo + g.columns - depth
            for j in range(depth):
                for i in range(g.rows // SUB):
                    at = (g.row_halo + SUB * i) * g.width + g.at(first + j)
                    strips[side, j, pl.ds(SUB * i, SUB), :] = arr[
                        pl.ds(at, SUB, stride=g.width), :
                    ]
        start(trade, DIRS[4:])
        start(trade, DIRS[2:4])
        for side in range(2):
            first = g.row_halo if side == 0 else g.row_halo + g.rows - depth
            for i in range(depth):
                for k in range(g.pieces):
                    sides[side, i, pl.ds(k, SUB, stride=g.pieces), :] = piece(arr, g, first + i, k)
        start(trade, DIRS[:2])

    def send_raw(name, value):
        trade = trades[name]
        t, g, depth, sides, strips, rows, columns, corners = trade
        for side in range(2):
            first = g.column_halo if side == 0 else g.column_halo + g.columns - depth
            for j in range(depth):
                for i in range(g.rows // SUB):
                    strips[side, j, pl.ds(SUB * i, SUB), :] = value(
                        lambda ref: ref[pl.ds(SUB * i * g.width + first + j, SUB, stride=g.width), :]
                    )
        start(trade, DIRS[4:])
        start(trade, DIRS[2:4])
        for side in range(2):
            first = 0 if side == 0 else g.rows - depth
            for i in range(depth):
                for c in range(g.columns // SUB):
                    at = g.column_halo + SUB * c
                    sides[side, i, pl.ds(at, SUB), :] = value(
                        lambda ref: ref[pl.ds((first + i) * g.width + at, SUB), :]
                    )
        start(trade, DIRS[:2])

    def receive(name, arr):
        trade = trades[name]
        t, g, depth, sides, strips, rows, columns, corners = trade
        for q in DIRS:
            @pl.when(exists(q))
            def _():
                copy_of(trade, q, False).wait_send()
                copy_of(trade, q, True).wait_recv()
        for side in range(2):
            first = g.row_halo - depth if side == 0 else g.row_halo + g.rows
            for i in range(depth):
                for k in range(g.pieces):
                    put(arr, g, first + i, k, rows[side, i, pl.ds(k, SUB, stride=g.pieces), :])
        for side in range(2):
            first = g.column_halo - depth if side == 0 else g.column_halo + g.columns
            for j in range(depth):
                place = g.at(first + j)
                for i in range(g.rows // SUB):
                    at = (g.row_halo + SUB * i) * g.width + place
                    arr[pl.ds(at, SUB, stride=g.width), :] = columns[
                        side, j, pl.ds(SUB * i, SUB), :
                    ]
                for end in range(2):
                    row = g.row_halo - depth if end == 0 else g.row_halo + g.rows
                    skip = SUB - depth if end == 0 else 0
                    arr[pl.ds(row * g.width + place, depth, stride=g.width), :] = corners[
                        end * 2 + side, j, pl.ds(skip, depth), :
                    ]

    def piece(ref, g, row, k):
        return ref[pl.ds(pl.multiple_of(row * g.width + k * SUB, SUB), SUB), :]

    def put(ref, g, row, k, value):
        ref[pl.ds(pl.multiple_of(row * g.width + k * SUB, SUB), SUB), :] = value

    def around(ref, g, row):
        here = [piece(ref, g, row, k) for k in range(g.pieces)]
        before = [pltpu.roll(here[-1], 1, 0)] + here[:-1]
        after = here[1:] + [pltpu.roll(here[0], SUB - 1, 0)]
        sums = [
            (piece(ref, g, row - 1, k) + piece(ref, g, row + 1, k)) + (before[k] + after[k])
            for k in range(g.pieces)
        ]
        return here, sums

    def block(g, old, new, weight, load, row, count, ks):
        seen = {}

        def get(i, k):
            if (i, k) not in seen:
                seen[i, k] = piece(old, g, row + i, k)
            return seen[i, k]

        for k in ks:
            for i in range(count):
                left = get(i, k - 1) if k else pltpu.roll(get(i, g.pieces - 1), 1, 0)
                right = get(i, k + 1) if k < g.pieces - 1 else pltpu.roll(get(i, 0), SUB - 1, 0)
                total = (get(i - 1, k) + get(i + 1, k)) + (left + right)
                value = (
                    0.2 * get(i, k)
                    + piece(load, g, row + i, k)
                    + piece(weight, g, row + i, k) * total
                )
                if new is out:
                    at = (row + i - g.row_halo) * g.width + k
                    new[pl.ds(at, SUB, stride=g.pieces), :] = value
                else:
                    put(new, g, row + i, k, value)

    def part(g, old, new, weight, load, first, last, ks):
        whole = (last - first) // BLOCK

        @pl.loop(0, whole)
        def _(b):
            block(g, old, new, weight, load, first + BLOCK * b, BLOCK, ks)

        if last - first > whole * BLOCK:
            at = first + whole * BLOCK
            block(g, old, new, weight, load, at, last - at, ks)

    def sweep(g, old, new, weight, load, wider):
        part(g, old, new, weight, load, g.row_halo - wider, g.row_halo + g.rows + wider, range(g.pieces))

    def near(g, outside, inside):
        low = range(g.column_halo - outside, g.column_halo + inside)
        high = range(g.column_halo + g.columns - inside, g.column_halo + g.columns + outside)
        return sorted({c % g.pieces for c in (*low, *high)})

    def edges(g, old, new, weight, load, outside, inside):
        top, end = g.row_halo, g.row_halo + g.rows
        every = range(g.pieces)
        block(g, old, new, weight, load, top - outside, outside + inside, every)
        block(g, old, new, weight, load, end - inside, outside + inside, every)
        part(g, old, new, weight, load, top + inside, end - inside, near(g, outside, inside))

    def inner(g, old, new, weight, load, inside):
        ks = sorted(set(range(g.pieces)) - set(near(g, 0, inside)))
        first, last = g.row_halo + inside, g.row_halo + g.rows - inside
        part(g, old, new, weight, load, first, last, ks)

    loads[2].wait()
    send_raw("u_first", lambda read: read(raw[2]))
    loads[0].wait()
    send_raw("w", lambda read: 0.8 / (4.0 + read(raw[0])))
    loads[1].wait()
    send_raw("f", lambda read: 0.8 / (4.0 + read(raw[0])) * read(raw[1]))

    @pl.loop(0, coarse.rows)
    def _(row):
        total = [0.0] * coarse.pieces
        for half in range(RATIO):
            at = RATIO * row + half
            for k in range(fine.pieces):
                g4 = 4.0 + raw[0][pl.ds(at * fine.width + k, SUB, stride=fine.pieces), :]
                put(w, fine, at + fine.row_halo, k, 0.8 / g4)
                put(iw, fine, at, k, 1.25 * g4)
                total[k // RATIO] = total[k // RATIO] + g4
        for k in range(coarse.pieces):
            mean = total[k] * (1.0 / RATIO) - (4.0 * RATIO - 4.0)
            put(cw, coarse, row + coarse.row_halo, k, 0.8 / mean)

    send("cw", cw)

    @pl.loop(0, fine.rows, unroll=2)
    def _(row):
        for k in range(fine.pieces):
            put(u, fine, row + fine.row_halo, k, raw[2][pl.ds(row * fine.width + k, SUB, stride=fine.pieces), :])


    @pl.loop(0, fine.rows, unroll=2)
    def _(row):
        for k in range(fine.pieces):
            at = row + fine.row_halo
            put(f, fine, at, k, piece(w, fine, at, k) * raw[1][pl.ds(row * fine.width + k, SUB, stride=fine.pieces), :])

    sweep(fine, u, v, w, f, 0)
    receive("w", w)
    receive("u_first", u)
    receive("f", f)
    edges(fine, u, v, w, f, 1, 1)
    edges(fine, v, u, w, f, 0, 2)
    send("u_second", u)
    inner(fine, v, u, w, f, 2)
    sweep(fine, u, v, w, f, 0)
    receive("u_second", u)
    edges(fine, u, v, w, f, 1, 1)

    @pl.loop(0, coarse.rows)
    def _(row):
        total = [0.0] * coarse.pieces
        for half in range(RATIO):
            at = RATIO * row + half + fine.row_halo
            here, sums = around(v, fine, at)
            for k in range(fine.pieces):
                change = piece(f, fine, at, k) + piece(w, fine, at, k) * sums[k] - 0.8 * here[k]
                total[k // RATIO] = total[k // RATIO] + change * piece(
                    iw, fine, at - fine.row_halo, k
                )
        for k in range(coarse.pieces):
            at = row + coarse.row_halo
            put(cf, coarse, at, k, total[k] * (1.0 / RATIO) * piece(cw, coarse, at, k))

    send("cf", cf)
    receive("cw", cw)
    receive("cf", cf)
    old, new, spare = cf, ca, cb
    left = INNER - 1
    wider = 7
    while wider > 0:
        wider -= 1
        sweep(coarse, old, new, cw, cf, wider)
        old, new, spare = new, spare, new
        left -= 1
    send("cu", old)
    receive("cu", old)
    new = ca if old is cb else cb
    wider = 6
    while left > 0:
        wider -= 1
        sweep(coarse, old, new, cw, cf, wider)
        old, new = new, old
        left -= 1

    @pl.loop(-1, coarse.rows + 1)
    def _(row):
        for k in range(coarse.pieces):
            more = piece(old, coarse, row + coarse.row_halo, k)
            for half in range(RATIO):
                at = RATIO * row + half + fine.row_halo
                for part in range(RATIO):
                    put(v, fine, at, RATIO * k + part, piece(v, fine, at, RATIO * k + part) + more)

    edges(fine, v, u, w, f, 0, 2)
    send("u_third", u)
    inner(fine, v, u, w, f, 2)
    sweep(fine, u, v, w, f, 0)
    receive("u_third", u)
    edges(fine, u, v, w, f, 1, 1)
    stores = []
    chunk = fine.rows // CHUNKS
    for c in range(CHUNKS):
        first = fine.row_halo + c * chunk
        part(fine, v, out, w, f, first, first + chunk, range(fine.pieces))
        stores.append(
            pltpu.make_async_copy(
                out.reshape(fine.rows, fine.width, 128).at[
                    pl.ds(c * chunk, chunk), pl.ds(fine.column_halo, fine.columns), :
                ],
                out_hbm.at[pl.ds(c * chunk, chunk)],
                out_sem.at[c],
            )
        )
        stores[-1].start()
    for store in stores:
        store.wait()


def per_device(source_terms, initial_values, absorption):
    rows, columns, cases = source_terms.shape
    fine = Grid(rows, columns, ROWS, RATIO * HALO)
    coarse = Grid(rows // RATIO, columns // RATIO, HALO, HALO)
    grids = {"fine": fine, "coarse": coarse}

    def held(*shape):
        return pltpu.VMEM(shape + (cases,), jnp.float32)

    shapes = [held(rows * fine.width) for _ in range(3)]
    shapes += [held(fine.stored) for _ in range(4)]
    shapes += [held(rows * fine.width), held(rows * fine.width)]
    shapes += [held(coarse.stored) for _ in range(4)]
    count = len(TRADES) * len(DIRS)
    shapes += [
        pltpu.SemaphoreType.DMA((3,)),
        pltpu.SemaphoreType.DMA((CHUNKS,)),
        pltpu.SemaphoreType.DMA((count,)),
        pltpu.SemaphoreType.DMA((count,)),
    ]
    for name, which, depth in TRADES:
        g = grids[which]
        shapes += [
            held(2, depth, g.width),
            held(2, depth, g.rows),
            held(2, depth, g.width),
            held(2, depth, g.rows),
            held(4, depth, SUB),
        ]
    return pl.pallas_call(
        functools.partial(kernel, grids),
        out_shape=jax.ShapeDtypeStruct(source_terms.shape, jnp.float32),
        in_specs=[pl.BlockSpec(memory_space=pl.ANY)] * 3,
        out_specs=pl.BlockSpec(memory_space=pl.ANY),
        scratch_shapes=shapes,
        compiler_params=pltpu.CompilerParams(
            collective_id=0, has_side_effects=True, vmem_limit_bytes=60 * 1024 * 1024
        ),
    )(source_terms, initial_values, absorption)


def solution(mesh):
    placed = P(("shift", "band"), "lane", None)
    return jax.shard_map(
        per_device,
        mesh=mesh,
        in_specs=(placed, placed, placed),
        out_specs=placed,
        check_vma=False,
    )
```

```python
import functools

import jax
import jax.numpy as jnp
from jax import lax
from jax.experimental import pallas as pl
from jax.experimental.pallas import tpu as pltpu
from jax.sharding import PartitionSpec as P

RATIO = 2
BEFORE = 3
AFTER = 3
INNER = 13
HALO = 8
ROWS = 2
SUB = 8
MESH = pl.DeviceIdType.MESH
CHUNKS = 4
BLOCK = 4
DIRS = [(-1, 0), (1, 0), (0, -1), (0, 1), (-1, -1), (-1, 1), (1, -1), (1, 1)]

TRADES = [
    ("u_first", "fine", 2),
    ("w", "fine", 1),
    ("f", "fine", 1),
    ("cw", "coarse", 6),
    ("u_second", "fine", 2),
    ("cf", "coarse", 7),
    ("cu", "coarse", 6),
    ("u_third", "fine", 2),
]


class Grid:
    def __init__(self, rows, columns, row_halo, column_halo):
        self.rows, self.columns = rows, columns
        self.row_halo, self.column_halo = row_halo, column_halo
        self.pieces = (columns + 2 * column_halo) // SUB
        self.width = self.pieces * SUB
        self.stored = (rows + 2 * row_halo) * self.width

    def at(self, column):
        return (column % self.pieces) * SUB + column // self.pieces


def kernel(grids, src_hbm, init_hbm, abs_hbm, out_hbm, *scratch):
    fine, coarse = grids["fine"], grids["coarse"]
    raw = scratch[:3]
    u, v, w, f, iw, out, cw, cf, ca, cb, in_sem, out_sem, send_sem, recv_sem = scratch[3:17]
    lands = scratch[17:]
    band, lane = lax.axis_index("band"), lax.axis_index("lane")
    bands, lanes = lax.axis_size("band"), lax.axis_size("lane")

    def exists(q):
        dy, dx = q
        there = jnp.bool_(True)
        if dy:
            there = (band > 0) if dy < 0 else (band < bands - 1)
        if dx:
            beside = (lane > 0) if dx < 0 else (lane < lanes - 1)
            there = beside if not dy else there & beside
        return there

    def name_of(q):
        return {"band": band + q[0], "lane": lane + q[1]}

    loads = [
        pltpu.make_async_copy(
            ref,
            raw[i].reshape(fine.rows, fine.width, 128).at[:, pl.ds(fine.column_halo, fine.columns), :],
            in_sem.at[i],
        )
        for i, ref in enumerate((abs_hbm, src_hbm, init_hbm))
    ]
    for i in (2, 0, 1):
        loads[i].start()

    trades = {}
    for t, (name, which, depth) in enumerate(TRADES):
        trades[name] = (t, grids[which], depth) + tuple(lands[5 * t : 5 * t + 5])

    barrier = pltpu.get_barrier_semaphore()
    for q in DIRS:
        @pl.when(exists(q))
        def _():
            pl.semaphore_signal(barrier, inc=1, device_id=name_of(q), device_id_type=MESH)

    def landing(trade, q):
        t, g, depth, sides, strips, rows, columns, corners = trade
        dy, dx = q
        if not dx:
            return rows.at[(dy + 1) // 2, :, pl.ds(g.column_halo, g.columns), :]
        if not dy:
            return columns.at[(dx + 1) // 2]
        return corners.at[(dy + 1) // 2 * 2 + (dx + 1) // 2]

    def source(trade, q):
        t, g, depth, sides, strips, rows, columns, corners = trade
        dy, dx = q
        if not dx:
            return sides.at[(dy + 1) // 2, :, pl.ds(g.column_halo, g.columns), :]
        strip = strips.at[(dx + 1) // 2]
        if not dy:
            return strip
        return strip.at[:, pl.ds(0 if dy < 0 else g.rows - SUB, SUB), :]

    for trade in trades.values():
        for q in DIRS:
            @pl.when(jnp.logical_not(exists(q)))
            def _():
                ref = landing(trade, q)
                ref[...] = jnp.zeros(ref.shape, jnp.float32)

    on_band = (band > 0).astype(jnp.int32) + (band < bands - 1).astype(jnp.int32)
    on_lane = (lane > 0).astype(jnp.int32) + (lane < lanes - 1).astype(jnp.int32)
    pl.semaphore_wait(barrier, (on_band + 1) * (on_lane + 1) - 1)

    def copy_of(trade, q, arriving):
        t = trade[0]
        back = (-q[0], -q[1])
        i, j = DIRS.index(q), DIRS.index(back)
        return pltpu.make_async_remote_copy(
            src_ref=source(trade, q if not arriving else back),
            dst_ref=landing(trade, back if not arriving else q),
            send_sem=send_sem.at[t * 8 + i],
            recv_sem=recv_sem.at[t * 8 + (i if arriving else j)],
            device_id=name_of(q),
            device_id_type=MESH,
        )

    def start(trade, directions):
        for q in directions:
            @pl.when(exists(q))
            def _():
                copy_of(trade, q, False).start()

    def send(name, arr):
        trade = trades[name]
        t, g, depth, sides, strips, rows, columns, corners = trade
        for side in range(2):
            first = g.column_halo if side == 0 else g.column_halo + g.columns - depth
            for j in range(depth):
                for i in range(g.rows // SUB):
                    at = (g.row_halo + SUB * i) * g.width + g.at(first + j)
                    strips[side, j, pl.ds(SUB * i, SUB), :] = arr[
                        pl.ds(at, SUB, stride=g.width), :
                    ]
        start(trade, DIRS[4:])
        start(trade, DIRS[2:4])
        for side in range(2):
            first = g.row_halo if side == 0 else g.row_halo + g.rows - depth
            for i in range(depth):
                for k in range(g.pieces):
                    sides[side, i, pl.ds(k, SUB, stride=g.pieces), :] = piece(arr, g, first + i, k)
        start(trade, DIRS[:2])

    def send_raw(name, value):
        trade = trades[name]
        t, g, depth, sides, strips, rows, columns, corners = trade
        for side in range(2):
            first = g.column_halo if side == 0 else g.column_halo + g.columns - depth
            for j in range(depth):
                for i in range(g.rows // SUB):
                    strips[side, j, pl.ds(SUB * i, SUB), :] = value(
                        lambda ref: ref[pl.ds(SUB * i * g.width + first + j, SUB, stride=g.width), :]
                    )
        start(trade, DIRS[4:])
        start(trade, DIRS[2:4])
        for side in range(2):
            first = 0 if side == 0 else g.rows - depth
            for i in range(depth):
                for c in range(g.columns // SUB):
                    at = g.column_halo + SUB * c
                    sides[side, i, pl.ds(at, SUB), :] = value(
                        lambda ref: ref[pl.ds((first + i) * g.width + at, SUB), :]
                    )
        start(trade, DIRS[:2])

    def receive(name, arr):
        trade = trades[name]
        t, g, depth, sides, strips, rows, columns, corners = trade
        for q in DIRS:
            @pl.when(exists(q))
            def _():
                copy_of(trade, q, False).wait_send()
                copy_of(trade, q, True).wait_recv()
        for side in range(2):
            first = g.row_halo - depth if side == 0 else g.row_halo + g.rows
            for i in range(depth):
                for k in range(g.pieces):
                    put(arr, g, first + i, k, rows[side, i, pl.ds(k, SUB, stride=g.pieces), :])
        for side in range(2):
            first = g.column_halo - depth if side == 0 else g.column_halo + g.columns
            for j in range(depth):
                place = g.at(first + j)
                for i in range(g.rows // SUB):
                    at = (g.row_halo + SUB * i) * g.width + place
                    arr[pl.ds(at, SUB, stride=g.width), :] = columns[
                        side, j, pl.ds(SUB * i, SUB), :
                    ]
                for end in range(2):
                    row = g.row_halo - depth if end == 0 else g.row_halo + g.rows
                    skip = SUB - depth if end == 0 else 0
                    arr[pl.ds(row * g.width + place, depth, stride=g.width), :] = corners[
                        end * 2 + side, j, pl.ds(skip, depth), :
                    ]

    def piece(ref, g, row, k):
        return ref[pl.ds(pl.multiple_of(row * g.width + k * SUB, SUB), SUB), :]

    def put(ref, g, row, k, value):
        ref[pl.ds(pl.multiple_of(row * g.width + k * SUB, SUB), SUB), :] = value

    def around(ref, g, row):
        here = [piece(ref, g, row, k) for k in range(g.pieces)]
        before = [pltpu.roll(here[-1], 1, 0)] + here[:-1]
        after = here[1:] + [pltpu.roll(here[0], SUB - 1, 0)]
        sums = [
            (piece(ref, g, row - 1, k) + piece(ref, g, row + 1, k)) + (before[k] + after[k])
            for k in range(g.pieces)
        ]
        return here, sums

    def block(g, old, new, weight, load, row, count, ks):
        seen = {}

        def get(i, k):
            if (i, k) not in seen:
                seen[i, k] = piece(old, g, row + i, k)
            return seen[i, k]

        for k in ks:
            for i in range(count):
                left = get(i, k - 1) if k else pltpu.roll(get(i, g.pieces - 1), 1, 0)
                right = get(i, k + 1) if k < g.pieces - 1 else pltpu.roll(get(i, 0), SUB - 1, 0)
                total = (get(i - 1, k) + get(i + 1, k)) + (left + right)
                value = (
                    0.2 * get(i, k)
                    + piece(load, g, row + i, k)
                    + piece(weight, g, row + i, k) * total
                )
                if new is out:
                    at = (row + i - g.row_halo) * g.width + k
                    new[pl.ds(at, SUB, stride=g.pieces), :] = value
                else:
                    put(new, g, row + i, k, value)

    def part(g, old, new, weight, load, first, last, ks):
        whole = (last - first) // BLOCK

        @pl.loop(0, whole)
        def _(b):
            block(g, old, new, weight, load, first + BLOCK * b, BLOCK, ks)

        if last - first > whole * BLOCK:
            at = first + whole * BLOCK
            block(g, old, new, weight, load, at, last - at, ks)

    def sweep(g, old, new, weight, load, wider):
        part(g, old, new, weight, load, g.row_halo - wider, g.row_halo + g.rows + wider, range(g.pieces))

    def near(g, outside, inside):
        low = range(g.column_halo - outside, g.column_halo + inside)
        high = range(g.column_halo + g.columns - inside, g.column_halo + g.columns + outside)
        return sorted({c % g.pieces for c in (*low, *high)})

    def edges(g, old, new, weight, load, outside, inside):
        top, end = g.row_halo, g.row_halo + g.rows
        every = range(g.pieces)
        block(g, old, new, weight, load, top - outside, outside + inside, every)
        block(g, old, new, weight, load, end - inside, outside + inside, every)
        part(g, old, new, weight, load, top + inside, end - inside, near(g, outside, inside))

    def inner(g, old, new, weight, load, inside):
        ks = sorted(set(range(g.pieces)) - set(near(g, 0, inside)))
        first, last = g.row_halo + inside, g.row_halo + g.rows - inside
        part(g, old, new, weight, load, first, last, ks)

    loads[2].wait()
    send_raw("u_first", lambda read: read(raw[2]))
    loads[0].wait()
    send_raw("w", lambda read: 0.8 / (4.0 + read(raw[0])))
    loads[1].wait()
    send_raw("f", lambda read: 0.8 / (4.0 + read(raw[0])) * read(raw[1]))

    @pl.loop(0, coarse.rows)
    def _(row):
        total = [0.0] * coarse.pieces
        for half in range(RATIO):
            at = RATIO * row + half
            for k in range(fine.pieces):
                g4 = 4.0 + raw[0][pl.ds(at * fine.width + k, SUB, stride=fine.pieces), :]
                put(w, fine, at + fine.row_halo, k, 0.8 / g4)
                put(iw, fine, at, k, 1.25 * g4)
                total[k // RATIO] = total[k // RATIO] + g4
        for k in range(coarse.pieces):
            mean = total[k] * (1.0 / RATIO) - (4.0 * RATIO - 4.0)
            put(cw, coarse, row + coarse.row_halo, k, 0.8 / mean)

    send("cw", cw)

    @pl.loop(0, fine.rows, unroll=2)
    def _(row):
        for k in range(fine.pieces):
            put(u, fine, row + fine.row_halo, k, raw[2][pl.ds(row * fine.width + k, SUB, stride=fine.pieces), :])


    @pl.loop(0, fine.rows, unroll=2)
    def _(row):
        for k in range(fine.pieces):
            at = row + fine.row_halo
            put(f, fine, at, k, piece(w, fine, at, k) * raw[1][pl.ds(row * fine.width + k, SUB, stride=fine.pieces), :])

    sweep(fine, u, v, w, f, 0)
    receive("w", w)
    receive("u_first", u)
    receive("f", f)
    edges(fine, u, v, w, f, 1, 1)
    edges(fine, v, u, w, f, 0, 2)
    send("u_second", u)
    inner(fine, v, u, w, f, 2)
    sweep(fine, u, v, w, f, 0)
    receive("u_second", u)
    edges(fine, u, v, w, f, 1, 1)

    @pl.loop(0, coarse.rows)
    def _(row):
        total = [0.0] * coarse.pieces
        for half in range(RATIO):
            at = RATIO * row + half + fine.row_halo
            here, sums = around(v, fine, at)
            for k in range(fine.pieces):
                change = piece(f, fine, at, k) + piece(w, fine, at, k) * sums[k] - 0.8 * here[k]
                total[k // RATIO] = total[k // RATIO] + change * piece(
                    iw, fine, at - fine.row_halo, k
                )
        for k in range(coarse.pieces):
            at = row + coarse.row_halo
            put(cf, coarse, at, k, total[k] * (1.0 / RATIO) * piece(cw, coarse, at, k))

    send("cf", cf)
    receive("cw", cw)
    receive("cf", cf)
    old, new, spare = cf, ca, cb
    left = INNER - 1
    wider = 7
    while wider > 0:
        wider -= 1
        sweep(coarse, old, new, cw, cf, wider)
        old, new, spare = new, spare, new
        left -= 1
    send("cu", old)
    receive("cu", old)
    new = ca if old is cb else cb
    wider = 6
    while left > 0:
        wider -= 1
        sweep(coarse, old, new, cw, cf, wider)
        old, new = new, old
        left -= 1

    @pl.loop(-1, coarse.rows + 1)
    def _(row):
        for k in range(coarse.pieces):
            more = piece(old, coarse, row + coarse.row_halo, k)
            for half in range(RATIO):
                at = RATIO * row + half + fine.row_halo
                for part in range(RATIO):
                    put(v, fine, at, RATIO * k + part, piece(v, fine, at, RATIO * k + part) + more)

    edges(fine, v, u, w, f, 0, 2)
    send("u_third", u)
    inner(fine, v, u, w, f, 2)
    sweep(fine, u, v, w, f, 0)
    receive("u_third", u)
    edges(fine, u, v, w, f, 1, 1)
    chunk = fine.rows // CHUNKS
    for c in range(CHUNKS):
        first = fine.row_halo + c * chunk
        part(fine, v, out, w, f, first, first + chunk, range(fine.pieces))

        @pl.loop(c * chunk, (c + 1) * chunk, unroll=4)
        def _(row):
            at = pl.multiple_of(row * fine.width + fine.column_halo, SUB)
            out_hbm[row] = out[pl.ds(at, fine.columns), :]


def per_device(source_terms, initial_values, absorption):
    rows, columns, cases = source_terms.shape
    fine = Grid(rows, columns, ROWS, RATIO * HALO)
    coarse = Grid(rows // RATIO, columns // RATIO, HALO, HALO)
    grids = {"fine": fine, "coarse": coarse}

    def held(*shape):
        return pltpu.VMEM(shape + (cases,), jnp.float32)

    shapes = [held(rows * fine.width) for _ in range(3)]
    shapes += [held(fine.stored) for _ in range(4)]
    shapes += [held(rows * fine.width), held(rows * fine.width)]
    shapes += [held(coarse.stored) for _ in range(4)]
    count = len(TRADES) * len(DIRS)
    shapes += [
        pltpu.SemaphoreType.DMA((3,)),
        pltpu.SemaphoreType.DMA((CHUNKS,)),
        pltpu.SemaphoreType.DMA((count,)),
        pltpu.SemaphoreType.DMA((count,)),
    ]
    for name, which, depth in TRADES:
        g = grids[which]
        shapes += [
            held(2, depth, g.width),
            held(2, depth, g.rows),
            held(2, depth, g.width),
            held(2, depth, g.rows),
            held(4, depth, SUB),
        ]
    return pl.pallas_call(
        functools.partial(kernel, grids),
        out_shape=jax.ShapeDtypeStruct(source_terms.shape, jnp.float32),
        in_specs=[pl.BlockSpec(memory_space=pltpu.HBM)] * 3,
        out_specs=pl.BlockSpec(memory_space=pltpu.VMEM),
        scratch_shapes=shapes,
        compiler_params=pltpu.CompilerParams(
            collective_id=0, has_side_effects=True, vmem_limit_bytes=44 * 1024 * 1024
        ),
    )(*[pltpu.with_memory_space_constraint(x, pltpu.HBM) for x in (source_terms, initial_values, absorption)])


def solution(mesh):
    placed = P(("shift", "band"), "lane", None)
    return jax.shard_map(
        per_device,
        mesh=mesh,
        in_specs=(placed, placed, placed),
        out_specs=placed,
        check_vma=False,
    )
```

```python
import functools

import jax
import jax.numpy as jnp
from jax import lax
from jax.experimental import pallas as pl
from jax.experimental.pallas import tpu as pltpu
from jax.sharding import PartitionSpec as P

RATIO = 2
BEFORE = 3
AFTER = 3
INNER = 13
HALO = 8
ROWS = 2
SUB = 8
MESH = pl.DeviceIdType.MESH
CHUNKS = 4
BLOCK = 8
DIRS = [(-1, 0), (1, 0), (0, -1), (0, 1), (-1, -1), (-1, 1), (1, -1), (1, 1)]

TRADES = [
    ("u_first", "fine", 2),
    ("w", "fine", 1),
    ("f", "fine", 1),
    ("cw", "coarse", 6),
    ("u_second", "fine", 2),
    ("cf", "coarse", 7),
    ("cu", "coarse", 6),
    ("u_third", "fine", 2),
]


class Grid:
    def __init__(self, rows, columns, row_halo, column_halo):
        self.rows, self.columns = rows, columns
        self.row_halo, self.column_halo = row_halo, column_halo
        self.pieces = (columns + 2 * column_halo) // SUB
        self.width = self.pieces * SUB
        self.stored = (rows + 2 * row_halo) * self.width

    def at(self, column):
        return (column % self.pieces) * SUB + column // self.pieces


def kernel(grids, src_hbm, init_hbm, abs_hbm, out_hbm, *scratch):
    fine, coarse = grids["fine"], grids["coarse"]
    raw = scratch[:3]
    u, v, w, f, iw, out, cw, cf, ca, cb, in_sem, out_sem, send_sem, recv_sem = scratch[3:17]
    lands = scratch[17:]
    band, lane = lax.axis_index("band"), lax.axis_index("lane")
    bands, lanes = lax.axis_size("band"), lax.axis_size("lane")

    def exists(q):
        dy, dx = q
        there = jnp.bool_(True)
        if dy:
            there = (band > 0) if dy < 0 else (band < bands - 1)
        if dx:
            beside = (lane > 0) if dx < 0 else (lane < lanes - 1)
            there = beside if not dy else there & beside
        return there

    def name_of(q):
        return {"band": band + q[0], "lane": lane + q[1]}

    loads = [
        pltpu.make_async_copy(
            ref,
            raw[i].reshape(fine.rows, fine.width, 128).at[:, pl.ds(fine.column_halo, fine.columns), :],
            in_sem.at[i],
        )
        for i, ref in enumerate((abs_hbm, src_hbm, init_hbm))
    ]
    for i in (2, 0, 1):
        loads[i].start()

    trades = {}
    for t, (name, which, depth) in enumerate(TRADES):
        trades[name] = (t, grids[which], depth) + tuple(lands[5 * t : 5 * t + 5])

    barrier = pltpu.get_barrier_semaphore()
    for q in DIRS:
        @pl.when(exists(q))
        def _():
            pl.semaphore_signal(barrier, inc=1, device_id=name_of(q), device_id_type=MESH)

    def landing(trade, q):
        t, g, depth, sides, strips, rows, columns, corners = trade
        dy, dx = q
        if not dx:
            return rows.at[(dy + 1) // 2, :, pl.ds(g.column_halo, g.columns), :]
        if not dy:
            return columns.at[(dx + 1) // 2]
        return corners.at[(dy + 1) // 2 * 2 + (dx + 1) // 2]

    def source(trade, q):
        t, g, depth, sides, strips, rows, columns, corners = trade
        dy, dx = q
        if not dx:
            return sides.at[(dy + 1) // 2, :, pl.ds(g.column_halo, g.columns), :]
        strip = strips.at[(dx + 1) // 2]
        if not dy:
            return strip
        return strip.at[:, pl.ds(0 if dy < 0 else g.rows - SUB, SUB), :]

    for trade in trades.values():
        for q in DIRS:
            @pl.when(jnp.logical_not(exists(q)))
            def _():
                ref = landing(trade, q)
                ref[...] = jnp.zeros(ref.shape, jnp.float32)

    on_band = (band > 0).astype(jnp.int32) + (band < bands - 1).astype(jnp.int32)
    on_lane = (lane > 0).astype(jnp.int32) + (lane < lanes - 1).astype(jnp.int32)
    pl.semaphore_wait(barrier, (on_band + 1) * (on_lane + 1) - 1)

    def copy_of(trade, q, arriving):
        t = trade[0]
        back = (-q[0], -q[1])
        i, j = DIRS.index(q), DIRS.index(back)
        return pltpu.make_async_remote_copy(
            src_ref=source(trade, q if not arriving else back),
            dst_ref=landing(trade, back if not arriving else q),
            send_sem=send_sem.at[t * 8 + i],
            recv_sem=recv_sem.at[t * 8 + (i if arriving else j)],
            device_id=name_of(q),
            device_id_type=MESH,
        )

    def start(trade, directions):
        for q in directions:
            @pl.when(exists(q))
            def _():
                copy_of(trade, q, False).start()

    def send(name, arr):
        trade = trades[name]
        t, g, depth, sides, strips, rows, columns, corners = trade
        for side in range(2):
            first = g.column_halo if side == 0 else g.column_halo + g.columns - depth
            for j in range(depth):
                for i in range(g.rows // SUB):
                    at = (g.row_halo + SUB * i) * g.width + g.at(first + j)
                    strips[side, j, pl.ds(SUB * i, SUB), :] = arr[
                        pl.ds(at, SUB, stride=g.width), :
                    ]
        start(trade, DIRS[4:])
        start(trade, DIRS[2:4])
        for side in range(2):
            first = g.row_halo if side == 0 else g.row_halo + g.rows - depth
            for i in range(depth):
                for k in range(g.pieces):
                    sides[side, i, pl.ds(k, SUB, stride=g.pieces), :] = piece(arr, g, first + i, k)
        start(trade, DIRS[:2])

    def send_raw(name, value):
        trade = trades[name]
        t, g, depth, sides, strips, rows, columns, corners = trade
        for side in range(2):
            first = g.column_halo if side == 0 else g.column_halo + g.columns - depth
            for j in range(depth):
                for i in range(g.rows // SUB):
                    strips[side, j, pl.ds(SUB * i, SUB), :] = value(
                        lambda ref: ref[pl.ds(SUB * i * g.width + first + j, SUB, stride=g.width), :]
                    )
        start(trade, DIRS[4:])
        start(trade, DIRS[2:4])
        for side in range(2):
            first = 0 if side == 0 else g.rows - depth
            for i in range(depth):
                for c in range(g.columns // SUB):
                    at = g.column_halo + SUB * c
                    sides[side, i, pl.ds(at, SUB), :] = value(
                        lambda ref: ref[pl.ds((first + i) * g.width + at, SUB), :]
                    )
        start(trade, DIRS[:2])

    def receive(name, arr):
        trade = trades[name]
        t, g, depth, sides, strips, rows, columns, corners = trade
        for q in DIRS:
            @pl.when(exists(q))
            def _():
                copy_of(trade, q, False).wait_send()
                copy_of(trade, q, True).wait_recv()
        for side in range(2):
            first = g.row_halo - depth if side == 0 else g.row_halo + g.rows
            for i in range(depth):
                for k in range(g.pieces):
                    put(arr, g, first + i, k, rows[side, i, pl.ds(k, SUB, stride=g.pieces), :])
        for side in range(2):
            first = g.column_halo - depth if side == 0 else g.column_halo + g.columns
            for j in range(depth):
                place = g.at(first + j)
                for i in range(g.rows // SUB):
                    at = (g.row_halo + SUB * i) * g.width + place
                    arr[pl.ds(at, SUB, stride=g.width), :] = columns[
                        side, j, pl.ds(SUB * i, SUB), :
                    ]
                for end in range(2):
                    row = g.row_halo - depth if end == 0 else g.row_halo + g.rows
                    skip = SUB - depth if end == 0 else 0
                    arr[pl.ds(row * g.width + place, depth, stride=g.width), :] = corners[
                        end * 2 + side, j, pl.ds(skip, depth), :
                    ]

    def piece(ref, g, row, k):
        return ref[pl.ds(pl.multiple_of(row * g.width + k * SUB, SUB), SUB), :]

    def put(ref, g, row, k, value):
        ref[pl.ds(pl.multiple_of(row * g.width + k * SUB, SUB), SUB), :] = value

    def around(ref, g, row):
        here = [piece(ref, g, row, k) for k in range(g.pieces)]
        before = [pltpu.roll(here[-1], 1, 0)] + here[:-1]
        after = here[1:] + [pltpu.roll(here[0], SUB - 1, 0)]
        sums = [
            (piece(ref, g, row - 1, k) + piece(ref, g, row + 1, k)) + (before[k] + after[k])
            for k in range(g.pieces)
        ]
        return here, sums

    def block(g, old, new, weight, load, row, count, ks):
        seen = {}

        def get(i, k):
            if (i, k) not in seen:
                seen[i, k] = piece(old, g, row + i, k)
            return seen[i, k]

        for k in ks:
            for i in range(count):
                left = get(i, k - 1) if k else pltpu.roll(get(i, g.pieces - 1), 1, 0)
                right = get(i, k + 1) if k < g.pieces - 1 else pltpu.roll(get(i, 0), SUB - 1, 0)
                total = (get(i - 1, k) + get(i + 1, k)) + (left + right)
                value = (
                    0.2 * get(i, k)
                    + piece(load, g, row + i, k)
                    + piece(weight, g, row + i, k) * total
                )
                if new is out:
                    at = (row + i - g.row_halo) * g.width + k
                    new[pl.ds(at, SUB, stride=g.pieces), :] = value
                else:
                    put(new, g, row + i, k, value)

    def part(g, old, new, weight, load, first, last, ks):
        whole = (last - first) // BLOCK

        @pl.loop(0, whole)
        def _(b):
            block(g, old, new, weight, load, first + BLOCK * b, BLOCK, ks)

        if last - first > whole * BLOCK:
            at = first + whole * BLOCK
            block(g, old, new, weight, load, at, last - at, ks)

    def sweep(g, old, new, weight, load, wider):
        part(g, old, new, weight, load, g.row_halo - wider, g.row_halo + g.rows + wider, range(g.pieces))

    def near(g, outside, inside):
        low = range(g.column_halo - outside, g.column_halo + inside)
        high = range(g.column_halo + g.columns - inside, g.column_halo + g.columns + outside)
        return sorted({c % g.pieces for c in (*low, *high)})

    def edges(g, old, new, weight, load, outside, inside):
        top, end = g.row_halo, g.row_halo + g.rows
        every = range(g.pieces)
        block(g, old, new, weight, load, top - outside, outside + inside, every)
        block(g, old, new, weight, load, end - inside, outside + inside, every)
        part(g, old, new, weight, load, top + inside, end - inside, near(g, outside, inside))

    def inner(g, old, new, weight, load, inside):
        ks = sorted(set(range(g.pieces)) - set(near(g, 0, inside)))
        first, last = g.row_halo + inside, g.row_halo + g.rows - inside
        part(g, old, new, weight, load, first, last, ks)

    loads[2].wait()
    send_raw("u_first", lambda read: read(raw[2]))
    loads[0].wait()
    send_raw("w", lambda read: 0.8 / (4.0 + read(raw[0])))
    loads[1].wait()
    send_raw("f", lambda read: 0.8 / (4.0 + read(raw[0])) * read(raw[1]))

    @pl.loop(0, coarse.rows)
    def _(row):
        total = [0.0] * coarse.pieces
        for half in range(RATIO):
            at = RATIO * row + half
            for k in range(fine.pieces):
                g4 = 4.0 + raw[0][pl.ds(at * fine.width + k, SUB, stride=fine.pieces), :]
                put(w, fine, at + fine.row_halo, k, 0.8 / g4)
                put(iw, fine, at, k, 1.25 * g4)
                total[k // RATIO] = total[k // RATIO] + g4
        for k in range(coarse.pieces):
            mean = total[k] * (1.0 / RATIO) - (4.0 * RATIO - 4.0)
            put(cw, coarse, row + coarse.row_halo, k, 0.8 / mean)


    @pl.loop(0, fine.rows, unroll=2)
    def _(row):
        for k in range(fine.pieces):
            put(u, fine, row + fine.row_halo, k, raw[2][pl.ds(row * fine.width + k, SUB, stride=fine.pieces), :])


    @pl.loop(0, fine.rows, unroll=2)
    def _(row):
        for k in range(fine.pieces):
            at = row + fine.row_halo
            put(f, fine, at, k, piece(w, fine, at, k) * raw[1][pl.ds(row * fine.width + k, SUB, stride=fine.pieces), :])

    sweep(fine, u, v, w, f, 0)
    receive("w", w)
    receive("u_first", u)
    receive("f", f)
    edges(fine, u, v, w, f, 1, 1)
    edges(fine, v, u, w, f, 0, 2)
    send("u_second", u)
    send("cw", cw)
    inner(fine, v, u, w, f, 2)
    sweep(fine, u, v, w, f, 0)
    receive("u_second", u)
    edges(fine, u, v, w, f, 1, 1)

    @pl.loop(0, coarse.rows)
    def _(row):
        total = [0.0] * coarse.pieces
        for half in range(RATIO):
            at = RATIO * row + half + fine.row_halo
            here, sums = around(v, fine, at)
            for k in range(fine.pieces):
                change = piece(f, fine, at, k) + piece(w, fine, at, k) * sums[k] - 0.8 * here[k]
                total[k // RATIO] = total[k // RATIO] + change * piece(
                    iw, fine, at - fine.row_halo, k
                )
        for k in range(coarse.pieces):
            at = row + coarse.row_halo
            put(cf, coarse, at, k, total[k] * (1.0 / RATIO) * piece(cw, coarse, at, k))

    send("cf", cf)
    receive("cw", cw)
    receive("cf", cf)
    old, new, spare = cf, ca, cb
    left = INNER - 1
    wider = 7
    while wider > 0:
        wider -= 1
        sweep(coarse, old, new, cw, cf, wider)
        old, new, spare = new, spare, new
        left -= 1
    send("cu", old)
    receive("cu", old)
    new = ca if old is cb else cb
    wider = 6
    while left > 0:
        wider -= 1
        sweep(coarse, old, new, cw, cf, wider)
        old, new = new, old
        left -= 1

    @pl.loop(-1, coarse.rows + 1)
    def _(row):
        for k in range(coarse.pieces):
            more = piece(old, coarse, row + coarse.row_halo, k)
            for half in range(RATIO):
                at = RATIO * row + half + fine.row_halo
                for part in range(RATIO):
                    put(v, fine, at, RATIO * k + part, piece(v, fine, at, RATIO * k + part) + more)

    edges(fine, v, u, w, f, 0, 2)
    send("u_third", u)
    inner(fine, v, u, w, f, 2)
    sweep(fine, u, v, w, f, 0)
    receive("u_third", u)
    edges(fine, u, v, w, f, 1, 1)
    chunk = fine.rows // CHUNKS
    for c in range(CHUNKS):
        first = fine.row_halo + c * chunk
        part(fine, v, out, w, f, first, first + chunk, range(fine.pieces))

        @pl.loop(c * chunk, (c + 1) * chunk, unroll=4)
        def _(row):
            at = pl.multiple_of(row * fine.width + fine.column_halo, SUB)
            out_hbm[row] = out[pl.ds(at, fine.columns), :]


def per_device(source_terms, initial_values, absorption):
    rows, columns, cases = source_terms.shape
    fine = Grid(rows, columns, ROWS, RATIO * HALO)
    coarse = Grid(rows // RATIO, columns // RATIO, HALO, HALO)
    grids = {"fine": fine, "coarse": coarse}

    def held(*shape):
        return pltpu.VMEM(shape + (cases,), jnp.float32)

    shapes = [held(rows * fine.width) for _ in range(3)]
    shapes += [held(fine.stored) for _ in range(4)]
    shapes += [held(rows * fine.width), held(rows * fine.width)]
    shapes += [held(coarse.stored) for _ in range(4)]
    count = len(TRADES) * len(DIRS)
    shapes += [
        pltpu.SemaphoreType.DMA((3,)),
        pltpu.SemaphoreType.DMA((CHUNKS,)),
        pltpu.SemaphoreType.DMA((count,)),
        pltpu.SemaphoreType.DMA((count,)),
    ]
    for name, which, depth in TRADES:
        g = grids[which]
        shapes += [
            held(2, depth, g.width),
            held(2, depth, g.rows),
            held(2, depth, g.width),
            held(2, depth, g.rows),
            held(4, depth, SUB),
        ]
    return pl.pallas_call(
        functools.partial(kernel, grids),
        out_shape=jax.ShapeDtypeStruct(source_terms.shape, jnp.float32),
        in_specs=[pl.BlockSpec(memory_space=pltpu.HBM)] * 3,
        out_specs=pl.BlockSpec(memory_space=pltpu.VMEM),
        scratch_shapes=shapes,
        compiler_params=pltpu.CompilerParams(
            collective_id=0, has_side_effects=True, vmem_limit_bytes=44 * 1024 * 1024
        ),
    )(*[pltpu.with_memory_space_constraint(x, pltpu.HBM) for x in (source_terms, initial_values, absorption)])


def solution(mesh):
    placed = P(("shift", "band"), "lane", None)
    return jax.shard_map(
        per_device,
        mesh=mesh,
        in_specs=(placed, placed, placed),
        out_specs=placed,
        check_vma=False,
    )
```
